32 devices in a mesh: dp: 8 (over z, y), tensor: 4 (over x, core).
Axes of the slice: x: 2, y: 2, z: 4, core: 2. Of those that a mesh axis runs over, the one named last changes fastest.
Arguments:
- activations: bfloat16 [4096, 6144], P('dp', 'tensor'), may hold values from -6 to 6
- cotangent: bfloat16 [4096, 5120], P('dp'), may hold values from -0.09375 to 0.09375
- master: float32 [5120, 6144], P('dp', 'tensor'), may hold values from -0.078125 to 0.078125
- moment_one: float32 [5120, 6144], P('dp', 'tensor'), may hold values from -0.3 to 0.3
- moment_two: float32 [5120, 6144], P('dp', 'tensor'), may hold values from 0.0002 to 0.002
- prompts: bfloat16 [1536, 6144], P('dp', 'tensor'), may hold values from -6 to 6
Outputs:
- new_master: float32 [5120, 6144], P('dp', 'tensor')
- new_moment_one: float32 [5120, 6144], P('dp', 'tensor')
- new_moment_two: float32 [5120, 6144], P('dp', 'tensor')
- projected: bfloat16 [1536, 5120], P(('dp', 'tensor'))
The draws below stay inside these ranges and needn't reach their ends.
All inputs are finite; a program needn't handle non-finite values.
Results may differ from the reference program's by a relative error of at most 0.03.
Values may be sent and summed in bfloat16 or wider, within the bound.
No kernel may reach another device: no remote copies, remote signals or barrier semaphores. Data moves between devices by JAX's collectives and lax.ppermute only.
A program may use at most 128 MiB of HBM per device.

```python
import math
import jax
import jax.numpy as jnp
from jax import lax

D = 5120
TOK_DEV = 512
IN = 6144
TOKENS = 4096
PROMPTS = 1536
N_DP = 8
N_TENSOR = 4


def with_spikes(entries, own_key, source, target, parts, factor):
    def block_of(dim):
        return (jnp.arange(entries.shape[dim]) // (entries.shape[dim] // parts)).reshape((-1,) + (1,) * (entries.ndim - 1 - dim))

    one_side = jax.random.permutation(own_key, parts)[block_of(target)]
    other_side = (block_of(target) + parts // 2) % parts
    return jnp.where((block_of(source) == one_side) | (block_of(source) == other_side), factor * entries, entries)


def block_scale(own_key, shape, cuts, smallest, largest):
    def one(dim, parts):
        heights = jax.random.uniform(jax.random.fold_in(jax.random.fold_in(own_key, 6), dim), (parts,), jnp.float32, smallest / len(cuts), largest / len(cuts))
        return jnp.repeat(jnp.exp(heights), shape[dim] // parts).reshape((-1,) + (1,) * (len(shape) - dim - 1))

    factor_of = one(*cuts[0])
    for cut in cuts[1:]:
        factor_of = factor_of * one(*cut)
    return factor_of


def centred(rng, extent, spread, limit, shards=(), held_as=jnp.bfloat16):
    factor_of = block_scale(rng, extent, shards, -0.22, 0.18) if shards else 1.0
    entries = jax.random.normal(rng, extent, jnp.float32) * spread * factor_of
    return jnp.minimum(jnp.maximum(entries, -limit), limit).astype(held_as)


def heavy_noise(rng, shape, scale, most, shards, heavy, held_as=jnp.bfloat16):
    values = scale * jax.random.normal(rng, shape, jnp.float32)
    if shards:
        values = values * block_scale(rng, shape, shards, -0.22, 0.18)
    return jnp.clip(with_spikes(values, jax.random.fold_in(rng, 3), *heavy), -most, most).astype(held_as)


def setup_inputs(seed: int = 0) -> dict:
    seeds = jax.random.split(jax.random.key(seed), 7)
    activations = centred(seeds[0], (TOKENS, IN), 1.0, 6.0, ((0, 8), (1, 4)))
    cotangent = heavy_noise(seeds[1], (TOKENS, D), (TOKENS ** -0.5), 0.09375, ((0, 8),), (0, 1, 8, 2.0))
    master = centred(seeds[2], (D, IN), IN ** -0.5, 0.078125, ((0, 8), (1, 4)), jnp.float32)
    moment_one = centred(seeds[3], (D, IN), 0.05, 0.3, ((0, 8), (1, 4)), jnp.float32)
    moment_two = jnp.clip(jnp.exp(math.log(0.002) - 2.3025852 * jax.random.uniform(seeds[4], (D, IN), jnp.float32) ** block_scale(seeds[4], (D, IN), ((0, 8), (1, 4)), -0.2, 0.2)), 0.0002, 0.002)
    prompts = centred(seeds[5], (PROMPTS, IN), 1.0, 6.0, ((0, 8), (1, 4)))
    return dict(activations=activations, cotangent=cotangent, master=master, moment_one=moment_one, moment_two=moment_two, prompts=prompts)


def reference(activations, cotangent, master, moment_one, moment_two, prompts):
    act_blocks = activations.reshape(N_DP, TOK_DEV, IN)
    cot_blocks = cotangent.reshape(N_DP, TOK_DEV, D)

    def add_block(total, pair):
        acts, cots = pair
        term = lax.dot_general(cots, acts, (((0,), (0,)), ((), ())), preferred_element_type=jnp.float32)
        rounded = lax.optimization_barrier(term.astype(jnp.bfloat16))
        return (total + rounded.astype(jnp.float32), None)
    grad, _ = lax.scan(add_block, jnp.zeros((D, IN), jnp.float32), (act_blocks, cot_blocks))
    new_one = 0.9 * moment_one + 0.1 * grad
    new_two = 0.999 * moment_two + 0.001 * grad * grad
    first = new_one / (1.0 - 0.9 ** 50)
    second = new_two / (1.0 - 0.999 ** 50)
    new_master = master - 0.003 * (first / (jnp.sqrt(second) + 1e-08) + 0.01 * master)
    rollout_weight = new_master.astype(jnp.bfloat16)
    width = IN // N_TENSOR
    prompt_blocks = prompts.reshape(PROMPTS, N_TENSOR, width).transpose(1, 0, 2)
    weight_blocks = rollout_weight.reshape(D, N_TENSOR, width).transpose(1, 0, 2)

    def add_part(total, pair):
        rows, weights = pair
        part = lax.dot_general(rows, weights, (((1,), (1,)), ((), ())), preferred_element_type=jnp.float32)
        rounded = lax.optimization_barrier(part.astype(jnp.bfloat16))
        return (total + rounded.astype(jnp.float32), None)
    summed, _ = lax.scan(add_part, jnp.zeros((PROMPTS, D), jnp.float32), (prompt_blocks, weight_blocks))
    return (new_master, new_one, new_two, summed.astype(jnp.bfloat16))
```

```python
import functools
import math

import jax
import jax.numpy as jnp
from jax import lax
from jax.experimental import pallas as pl
from jax.experimental.pallas import tpu as pltpu
from jax.sharding import PartitionSpec as P


GROUP = 4
SHARE = 4
COLUMN_PARTS = 2
TILE = 128


def swap(x, axis, bit):
    n = lax.axis_size(axis)
    return lax.ppermute(x, axis, [(i, i ^ bit) for i in range(n)])


def dot_tokens(cot, acts):
    return lax.dot_general(cot, acts, (((0,), (0,)), ((), ())), preferred_element_type=jnp.float32)


def dot_features(rows, weight):
    return lax.dot_general(rows, weight, (((1,), (1,)), ((), ())), preferred_element_type=jnp.float32)


def row_parts(rows):
    if rows % 128:
        return [(0, rows)]
    first = (rows // 128 * 3 + 4) // 5 * 128
    return [(0, first), (first, rows - first)] if first < rows else [(0, rows)]


def adam_kernel(n_recv, *refs):
    own, recvs = refs[0], refs[1 : 1 + n_recv]
    master, one, two = refs[1 + n_recv : 4 + n_recv]
    new_master, new_one, new_two, weight = refs[-4:]
    grad = own[...]
    for recv in recvs:
        grad = grad + recv[...].astype(jnp.float32)
    first = 0.9 * one[...] + 0.1 * grad
    second = 0.999 * two[...] + 0.001 * grad * grad
    new_one[...] = first
    new_two[...] = second
    held = master[...]
    step = (first * (1.0 / (1.0 - 0.9**50))) / (jnp.sqrt(second * (1.0 / (1.0 - 0.999**50))) + 1e-08)
    updated = held - 0.003 * (step + 0.01 * held)
    new_master[...] = updated
    weight[...] = updated.astype(jnp.bfloat16)


def adam(own, recvs, state, previous, row, column):
    rows, width = recvs[0].shape if recvs else own.shape
    full = state[0].shape
    tile = math.gcd(math.gcd(rows, row), TILE) if rows % TILE == 0 else rows
    here = pl.BlockSpec((tile, width), lambda i: (i, 0))
    below = pl.BlockSpec((tile, width), lambda i: (i + row // tile, 0))
    there = pl.BlockSpec((tile, width), lambda i: (i + row // tile, column // width))
    held = list(previous) if previous is not None else []
    n_in = 1 + len(recvs) + 3
    return pl.pallas_call(
        functools.partial(adam_kernel, len(recvs)),
        grid=(rows // tile,),
        in_specs=[below] + [here] * len(recvs) + [there] * 3 + [pl.BlockSpec(memory_space=pl.ANY)] * len(held),
        out_specs=[there] * 3 + [here],
        out_shape=[jax.ShapeDtypeStruct(full, jnp.float32)] * 3 + [jax.ShapeDtypeStruct((rows, width), jnp.bfloat16)],
        input_output_aliases={n_in + j: j for j in range(len(held))},
        cost_estimate=pl.CostEstimate(flops=20 * rows * width, bytes_accessed=32 * rows * width, transcendentals=2 * rows * width),
        name="adam",
    )(own, *recvs, *state, *held)


def place_kernel(rows, starts, me, *refs):
    out = refs[-1]
    for start, blocks in zip(starts, refs):
        n, _, size = blocks.shape
        for p in range(n):
            out[:, p * rows + start : p * rows + start + size] = blocks[lax.bitwise_xor(me[0], p)]


def gate(x, after):
    return lax.optimization_barrier((x, after))[0]


def send_cotangent(cotangent, tokens, rows, me, share, order):
    k, m = me // GROUP, me % GROUP
    part = tokens // SHARE
    got = {}
    for s in (3, 2, 1):
        pieces = [
            lax.dynamic_slice(cotangent, (share * part, ((k ^ c) * GROUP + (m ^ s)) * rows), (part, rows)) for c in order
        ]
        got[s] = swap(jnp.concatenate(pieces, axis=1), "dp", s)
    return got


def join_shares(mine, across, both, share, rows):
    peers, part, width = mine.shape
    whole = jnp.zeros((peers, SHARE * part, width), mine.dtype)
    for offset, piece in ((0, mine), (2, across), (1, both[0]), (3, both[1])):
        whole = lax.dynamic_update_slice(whole, piece, (0, (share ^ offset) * part, 0))
    return [[whole[s, :, i : i + rows] for s in range(peers)] for i in range(0, width, rows)]


def reduce_over_tensor(accs, n, owned, t, marks):
    n_tensor, size = lax.axis_size("tensor"), accs[0].shape[1]
    if n_tensor & (n_tensor - 1):
        acc = jnp.concatenate(accs)
        grouped = acc.reshape(n, n_tensor, owned, size).transpose(1, 0, 2, 3).astype(jnp.bfloat16)
        return lax.psum_scatter(grouped, "tensor", scatter_dimension=0, tiled=True).reshape(n, owned, size)
    lefts, bit = [acc.reshape(-1, n_tensor, owned, size) for acc in accs], 1
    while bit < n_tensor:
        mine = (t // bit) % 2
        pairs = [left.reshape(left.shape[0], left.shape[1] // 2, 2, owned, size) for left in lefts]
        going = [lax.dynamic_index_in_dim(pair, 1 - mine, 2, keepdims=False).astype(jnp.bfloat16) for pair in pairs]
        going = jnp.concatenate(going)
        marks.append(going)
        came = swap(going, "tensor", bit).astype(jnp.float32)
        lefts, at = [], 0
        for pair in pairs:
            kept = lax.dynamic_index_in_dim(pair, mine, 2, keepdims=False)
            lefts.append(kept + came[at : at + kept.shape[0]])
            at += kept.shape[0]
        bit *= 2
    return jnp.concatenate([left.reshape(-1, owned, size).astype(jnp.bfloat16) for left in lefts])


def exchange_over_dp(blocks, seen, n):
    blocks = {q: blocks[i] for i, q in enumerate(seen)}
    bit = n // 2
    while bit:
        going = [q for q in range(n) if q & bit]
        came = swap(jnp.stack([blocks[q] for q in going]), "dp", bit)
        blocks.update({q: came[i] for i, q in enumerate(going)})
        bit //= 2
    return jnp.stack([blocks[q] for q in range(n)])


def local(activations, cotangent, master, moment_one, moment_two, prompts):
    n, n_tensor = lax.axis_size("dp"), lax.axis_size("tensor")
    me, t = lax.axis_index("dp"), lax.axis_index("tensor")
    k, m = me // GROUP, me % GROUP
    n_groups = n // GROUP
    tokens, width = activations.shape
    rows = master.shape[0]
    state = (master, moment_one, moment_two)
    part_width = width // COLUMN_PARTS
    order = [*range(1, n_groups), 0]

    share = t % SHARE
    away = order[:-1]
    got = send_cotangent(cotangent, tokens, rows, me, share, order)

    blocks = [activations[:, j * part_width : (j + 1) * part_width] for j in range(COLUMN_PARTS)]
    ahead = [swap(block, "dp", 1) for block in blocks]
    side = [swap(block, "dp", 2) for block in blocks]
    diagonal = [swap(beside, "dp", 1) for beside in side]

    mine_of = {
        tag: jnp.stack([got[s][:, low:high] for s in (1, 2, 3)])
        for tag, low, high in (("a", 0, len(away) * rows), ("h", len(away) * rows, len(order) * rows))
    }
    across_of = {tag: swap(mine, "tensor", 2) for tag, mine in mine_of.items()}

    def cotangents(tag, across):
        both = swap(jnp.stack([mine_of[tag], across]), "tensor", 1)
        return join_shares(mine_of[tag], across, both, share, rows)

    def group_sum(j, c, cots, after):
        own = lax.dynamic_slice(cotangent, (0, ((k ^ c) * GROUP + m) * rows), (tokens, rows))
        if after is not None:
            own = gate(own, after)
        acc = dot_tokens(own, blocks[j])
        firsts[j] = acc
        acc = acc + dot_tokens(cots[0], ahead[j]) + dot_tokens(cots[1], side[j])
        return acc + dot_tokens(cots[2], gate(diagonal[j], acc))

    firsts = {}
    last = COLUMN_PARTS - 1
    parts = row_parts(rows)
    cots_away = cotangents("a", across_of["a"])
    sent = [group_sum(0, c, cots_away[i], None).astype(jnp.bfloat16) for i, c in enumerate(away)]
    received = {(0, 0): [swap(x, "dp", c * GROUP) for x, c in zip(sent, away)]}
    mark, early_mark = sent[-1], firsts[0]

    cots_home = cotangents("h", gate(across_of["h"], mark))
    own_sums = [group_sum(0, 0, cots_home[0], mark)]
    for j in range(1, COLUMN_PARTS):
        sums = [group_sum(j, c, cots_away[i], mark) for i, c in enumerate(away)]
        for start, size in parts if j == last else [(0, rows)]:
            sent = [x[start : start + size].astype(jnp.bfloat16) for x in sums]
            received[j, start] = [swap(x, "dp", c * GROUP) for x, c in zip(sent, away)]
        mark = sent[-1]
        own_sums.append(group_sum(j, 0, cots_home[0], mark))

    seen, held, bit = [0], [prompts], n // 2
    while bit > 1:
        held.append(swap(jnp.concatenate(held) if len(held) > 1 else held[0], "dp", bit))
        if bit > 2:
            held[-1] = gate(held[-1], early_mark)
        seen += [q ^ bit for q in seen]
        bit //= 2
    near = jnp.concatenate(held[:-1])
    far = held[-1]

    near_other = swap(near, "dp", 1)
    new_state, weights = None, []
    for j in range(last):
        recvs = [gate(x, mark) for x in received[j, 0]]
        *new_state, weight = adam(own_sums[j], recvs, state, new_state, 0, j * part_width)
        weights.append(weight)
    far = gate(far, mark)
    far_other = swap(far, "dp", 1)
    seen += [q ^ 1 for q in seen]

    def early_part(some):
        return [dot_features(some[:, j * part_width : (j + 1) * part_width], weights[j]) for j in range(last)]

    def late_part(some, done, weight, start, size):
        return sum((e[:, start : start + size] for e in done), start=dot_features(some[:, last * part_width :], weight))

    most = jnp.concatenate([near, far, near_other])
    early = early_part(most)
    early_other, mark = None, early[-1]
    owned = prompts.shape[0] // n_tensor
    outs = []
    for start, size in parts:
        recvs = [gate(x, mark) for x in received[last, start]]
        *new_state, weight = adam(own_sums[last], recvs, state, new_state, start, last * part_width)
        acc = late_part(most, early, weight, start, size)
        if early_other is None:
            far_other = gate(far_other, acc)
            early_other = early_part(far_other)
        acc_other = late_part(far_other, early_other, weight, start, size)
        marks = []
        left = reduce_over_tensor([acc, acc_other], n, owned, t, marks)
        mark = marks[0] if marks else acc_other
        outs.append(exchange_over_dp(left, seen, n))
    projected = pl.pallas_call(
        functools.partial(place_kernel, rows, [start for start, _ in parts]),
        in_specs=[pl.BlockSpec(memory_space=pltpu.SMEM)] + [pl.BlockSpec(memory_space=pltpu.VMEM)] * len(outs),
        out_specs=pl.BlockSpec(memory_space=pltpu.VMEM),
        out_shape=jax.ShapeDtypeStruct((owned, n * rows), jnp.bfloat16),
        name="place",
    )(me.reshape(1), *outs)
    return (*new_state, projected)


def solution(mesh):
    placed = (
        P("dp", "tensor"),
        P("dp", None),
        P("dp", "tensor"),
        P("dp", "tensor"),
        P("dp", "tensor"),
        P("dp", "tensor"),
    )
    return jax.shard_map(
        local,
        mesh=mesh,
        in_specs=placed,
        out_specs=(
            P("dp", "tensor"),
            P("dp", "tensor"),
            P("dp", "tensor"),
            P(("dp", "tensor"), None),
        ),
        check_vma=False,
    )
```

```python
import functools
import math

import jax
import jax.numpy as jnp
from jax import lax
from jax.experimental import pallas as pl
from jax.experimental.pallas import tpu as pltpu
from jax.sharding import PartitionSpec as P


GROUP = 4
SHARE = 4
COLUMN_PARTS = 2
TILE = 128


def swap(x, axis, bit):
    n = lax.axis_size(axis)
    return lax.ppermute(x, axis, [(i, i ^ bit) for i in range(n)])


def dot_tokens(cot, acts):
    return lax.dot_general(cot, acts, (((0,), (0,)), ((), ())), preferred_element_type=jnp.float32)


def dot_features(rows, weight):
    return lax.dot_general(rows, weight, (((1,), (1,)), ((), ())), preferred_element_type=jnp.float32)


def row_parts(rows):
    if rows % 128:
        return [(0, rows)]
    first = (rows // 128 * 3 + 4) // 5 * 128
    return [(0, first), (first, rows - first)] if first < rows else [(0, rows)]


def adam_kernel(n_recv, *refs):
    own, recvs = refs[0], refs[1 : 1 + n_recv]
    master, one, two = refs[1 + n_recv : 4 + n_recv]
    new_master, new_one, new_two, weight = refs[-4:]
    grad = own[...]
    for recv in recvs:
        grad = grad + recv[...].astype(jnp.float32)
    first = 0.9 * one[...] + 0.1 * grad
    second = 0.999 * two[...] + 0.001 * grad * grad
    new_one[...] = first
    new_two[...] = second
    held = master[...]
    step = (first * (1.0 / (1.0 - 0.9**50))) / (jnp.sqrt(second * (1.0 / (1.0 - 0.999**50))) + 1e-08)
    updated = held - 0.003 * (step + 0.01 * held)
    new_master[...] = updated
    weight[...] = updated.astype(jnp.bfloat16)


def adam(own, recvs, state, previous, row, column):
    rows, width = recvs[0].shape if recvs else own.shape
    full = state[0].shape
    common = math.gcd(rows, row)
    tile = max(d for d in range(1, TILE + 1) if common % d == 0)
    here = pl.BlockSpec((tile, width), lambda i: (i, 0))
    below = pl.BlockSpec((tile, width), lambda i: (i + row // tile, 0))
    there = pl.BlockSpec((tile, width), lambda i: (i + row // tile, column // width))
    held = list(previous) if previous is not None else []
    n_in = 1 + len(recvs) + 3
    return pl.pallas_call(
        functools.partial(adam_kernel, len(recvs)),
        grid=(rows // tile,),
        in_specs=[below] + [here] * len(recvs) + [there] * 3 + [pl.BlockSpec(memory_space=pl.ANY)] * len(held),
        out_specs=[there] * 3 + [here],
        out_shape=[jax.ShapeDtypeStruct(full, jnp.float32)] * 3 + [jax.ShapeDtypeStruct((rows, width), jnp.bfloat16)],
        input_output_aliases={n_in + j: j for j in range(len(held))},
        cost_estimate=pl.CostEstimate(flops=20 * rows * width, bytes_accessed=32 * rows * width, transcendentals=2 * rows * width),
        name="adam",
    )(own, *recvs, *state, *held)


def place_kernel(rows, starts, me, *refs):
    out = refs[-1]
    for start, blocks in zip(starts, refs):
        n, _, size = blocks.shape
        for p in range(n):
            out[:, p * rows + start : p * rows + start + size] = blocks[lax.bitwise_xor(me[0], p)]


def gate(x, after):
    return lax.optimization_barrier((x, after))[0]


def send_cotangent(cotangent, tokens, rows, me, share, order):
    k, m = me // GROUP, me % GROUP
    part = tokens // SHARE
    got = {}
    for s in (3, 2, 1):
        pieces = [
            lax.dynamic_slice(cotangent, (share * part, ((k ^ c) * GROUP + (m ^ s)) * rows), (part, rows)) for c in order
        ]
        got[s] = swap(jnp.concatenate(pieces, axis=1), "dp", s)
    return got


def join_shares(mine, across, both, share, rows):
    peers, part, width = mine.shape
    whole = jnp.zeros((peers, SHARE * part, width), mine.dtype)
    for offset, piece in ((0, mine), (2, across), (1, both[0]), (3, both[1])):
        whole = lax.dynamic_update_slice(whole, piece, (0, (share ^ offset) * part, 0))
    return [[whole[s, :, i : i + rows] for s in range(peers)] for i in range(0, width, rows)]


def reduce_over_tensor(accs, n, owned, t, marks):
    n_tensor, size = lax.axis_size("tensor"), accs[0].shape[1]
    if n_tensor & (n_tensor - 1):
        acc = jnp.concatenate(accs)
        grouped = acc.reshape(n, n_tensor, owned, size).transpose(1, 0, 2, 3).astype(jnp.bfloat16)
        return lax.psum_scatter(grouped, "tensor", scatter_dimension=0, tiled=True).reshape(n, owned, size)
    lefts, bit = [acc.reshape(-1, n_tensor, owned, size) for acc in accs], 1
    while bit < n_tensor:
        mine = (t // bit) % 2
        pairs = [left.reshape(left.shape[0], left.shape[1] // 2, 2, owned, size) for left in lefts]
        going = [lax.dynamic_index_in_dim(pair, 1 - mine, 2, keepdims=False).astype(jnp.bfloat16) for pair in pairs]
        going = jnp.concatenate(going)
        marks.append(going)
        came = swap(going, "tensor", bit).astype(jnp.float32)
        lefts, at = [], 0
        for pair in pairs:
            kept = lax.dynamic_index_in_dim(pair, mine, 2, keepdims=False)
            lefts.append(kept + came[at : at + kept.shape[0]])
            at += kept.shape[0]
        bit *= 2
    return jnp.concatenate([left.reshape(-1, owned, size).astype(jnp.bfloat16) for left in lefts])


def exchange_over_dp(blocks, seen, n):
    blocks = {q: blocks[i] for i, q in enumerate(seen)}
    bit = n // 2
    while bit:
        going = [q for q in range(n) if q & bit]
        came = swap(jnp.stack([blocks[q] for q in going]), "dp", bit)
        blocks.update({q: came[i] for i, q in enumerate(going)})
        bit //= 2
    return jnp.stack([blocks[q] for q in range(n)])


def local(activations, cotangent, master, moment_one, moment_two, prompts):
    n, n_tensor = lax.axis_size("dp"), lax.axis_size("tensor")
    me, t = lax.axis_index("dp"), lax.axis_index("tensor")
    k, m = me // GROUP, me % GROUP
    n_groups = n // GROUP
    tokens, width = activations.shape
    rows = master.shape[0]
    state = (master, moment_one, moment_two)
    part_width = width // COLUMN_PARTS
    order = [*range(1, n_groups), 0]

    share = t % SHARE
    away = order[:-1]
    got = send_cotangent(cotangent, tokens, rows, me, share, order)

    blocks = [activations[:, j * part_width : (j + 1) * part_width] for j in range(COLUMN_PARTS)]
    ahead = [swap(block, "dp", 1) for block in blocks]
    side = [swap(block, "dp", 2) for block in blocks]
    diagonal = [swap(beside, "dp", 1) for beside in side]

    mine_of = {
        tag: jnp.stack([got[s][:, low:high] for s in (1, 2, 3)])
        for tag, low, high in (("a", 0, len(away) * rows), ("h", len(away) * rows, len(order) * rows))
    }
    across_of = {tag: swap(mine, "tensor", 2) for tag, mine in mine_of.items()}

    def cotangents(tag, across):
        both = swap(jnp.stack([mine_of[tag], across]), "tensor", 1)
        return join_shares(mine_of[tag], across, both, share, rows)

    def group_sum(j, c, cots, after):
        own = lax.dynamic_slice(cotangent, (0, ((k ^ c) * GROUP + m) * rows), (tokens, rows))
        if after is not None:
            own = gate(own, after)
        partial[j] = dot_tokens(own, blocks[j])
        acc = partial[j] + dot_tokens(cots[0], ahead[j]) + dot_tokens(cots[1], side[j])
        return acc + dot_tokens(cots[2], gate(diagonal[j], acc))

    partial = {}
    last = COLUMN_PARTS - 1
    parts = row_parts(rows)
    cots_away = cotangents("a", across_of["a"])
    sent = [group_sum(0, c, cots_away[i], None).astype(jnp.bfloat16) for i, c in enumerate(away)]
    received = {(0, 0): [swap(x, "dp", c * GROUP) for x, c in zip(sent, away)]}
    mark = sent[-1]

    cots_home = cotangents("h", gate(across_of["h"], mark))
    own_sums = [group_sum(0, 0, cots_home[0], mark)]
    for j in range(1, COLUMN_PARTS):
        sums = [group_sum(j, c, cots_away[i], mark) for i, c in enumerate(away)]
        for start, size in parts if j == last else [(0, rows)]:
            sent = [x[start : start + size].astype(jnp.bfloat16) for x in sums]
            received[j, start] = [swap(x, "dp", c * GROUP) for x, c in zip(sent, away)]
        mark, early_mark = sent[-1], partial[1]
        own_sums.append(group_sum(j, 0, cots_home[0], mark))

    seen, held, bit = [0], [prompts], n // 2
    while bit > 1:
        held.append(swap(jnp.concatenate(held) if len(held) > 1 else held[0], "dp", bit))
        if bit > 2:
            held[-1] = gate(held[-1], early_mark)
        seen += [q ^ bit for q in seen]
        bit //= 2
    near = jnp.concatenate(held[:-1])
    far = held[-1]

    near_other = swap(near, "dp", 1)
    mark = own_sums[-1]
    new_state, weights = None, []
    for j in range(last):
        recvs = [gate(x, mark) for x in received[j, 0]]
        *new_state, weight = adam(own_sums[j], recvs, state, new_state, 0, j * part_width)
        weights.append(weight)
    far = gate(far, weights[-1])
    far_other = swap(far, "dp", 1)
    seen += [q ^ 1 for q in seen]

    def early_part(some):
        return [dot_features(some[:, j * part_width : (j + 1) * part_width], weights[j]) for j in range(last)]

    def late_part(some, done, weight, start, size):
        return sum((e[:, start : start + size] for e in done), start=dot_features(some[:, last * part_width :], weight))

    most = jnp.concatenate([near, far, near_other])
    early = early_part(most)
    early_other, mark = None, early[-1]
    owned = prompts.shape[0] // n_tensor
    outs = []
    for start, size in parts:
        recvs = [gate(x, mark) for x in received[last, start]]
        *new_state, weight = adam(own_sums[last], recvs, state, new_state, start, last * part_width)
        acc = late_part(most, early, weight, start, size)
        if early_other is None:
            far_other = gate(far_other, acc)
            early_other = early_part(far_other)
        acc_other = late_part(far_other, early_other, weight, start, size)
        marks = []
        left = reduce_over_tensor([acc, acc_other], n, owned, t, marks)
        mark = marks[0] if marks else acc_other
        outs.append(exchange_over_dp(left, seen, n))
    projected = pl.pallas_call(
        functools.partial(place_kernel, rows, [start for start, _ in parts]),
        in_specs=[pl.BlockSpec(memory_space=pltpu.SMEM)] + [pl.BlockSpec(memory_space=pltpu.VMEM)] * len(outs),
        out_specs=pl.BlockSpec(memory_space=pltpu.VMEM),
        out_shape=jax.ShapeDtypeStruct((owned, n * rows), jnp.bfloat16),
        name="place",
    )(me.reshape(1), *outs)
    return (*new_state, projected)


def solution(mesh):
    placed = (
        P("dp", "tensor"),
        P("dp", None),
        P("dp", "tensor"),
        P("dp", "tensor"),
        P("dp", "tensor"),
        P("dp", "tensor"),
    )
    return jax.shard_map(
        local,
        mesh=mesh,
        in_specs=placed,
        out_specs=(
            P("dp", "tensor"),
            P("dp", "tensor"),
            P("dp", "tensor"),
            P(("dp", "tensor"), None),
        ),
        check_vma=False,
    )
```

```python
import functools
import math

import jax
import jax.numpy as jnp
from jax import lax
from jax.experimental import pallas as pl
from jax.experimental.pallas import tpu as pltpu
from jax.sharding import PartitionSpec as P


GROUP = 4
SHARE = 4
COLUMN_PARTS = 2
TILE = 128


def swap(x, axis, bit):
    n = lax.axis_size(axis)
    return lax.ppermute(x, axis, [(i, i ^ bit) for i in range(n)])


def dot_tokens(cot, acts):
    return lax.dot_general(cot, acts, (((0,), (0,)), ((), ())), preferred_element_type=jnp.float32)


def dot_features(rows, weight):
    return lax.dot_general(rows, weight, (((1,), (1,)), ((), ())), preferred_element_type=jnp.float32)


def row_parts(rows):
    if rows % 128:
        return [(0, rows)]
    first = (rows // 128 * 3 + 4) // 5 * 128
    return [(0, first), (first, rows - first)] if first < rows else [(0, rows)]


def adam_kernel(n_recv, *refs):
    own, recvs = refs[0], refs[1 : 1 + n_recv]
    master, one, two = refs[1 + n_recv : 4 + n_recv]
    new_master, new_one, new_two, weight = refs[-4:]
    grad = own[...]
    for recv in recvs:
        grad = grad + recv[...].astype(jnp.float32)
    first = 0.9 * one[...] + 0.1 * grad
    second = 0.999 * two[...] + 0.001 * grad * grad
    new_one[...] = first
    new_two[...] = second
    held = master[...]
    step = (first * (1.0 / (1.0 - 0.9**50))) / (jnp.sqrt(second * (1.0 / (1.0 - 0.999**50))) + 1e-08)
    updated = held - 0.003 * (step + 0.01 * held)
    new_master[...] = updated
    weight[...] = updated.astype(jnp.bfloat16)


def adam(own, recvs, state, previous, row, column):
    rows, width = recvs[0].shape if recvs else own.shape
    full = state[0].shape
    common = math.gcd(rows, row)
    tile = max(d for d in range(1, TILE + 1) if common % d == 0)
    here = pl.BlockSpec((tile, width), lambda i: (i, 0))
    below = pl.BlockSpec((tile, width), lambda i: (i + row // tile, 0))
    there = pl.BlockSpec((tile, width), lambda i: (i + row // tile, column // width))
    held = list(previous) if previous is not None else []
    n_in = 1 + len(recvs) + 3
    return pl.pallas_call(
        functools.partial(adam_kernel, len(recvs)),
        grid=(rows // tile,),
        in_specs=[below] + [here] * len(recvs) + [there] * 3 + [pl.BlockSpec(memory_space=pl.ANY)] * len(held),
        out_specs=[there] * 3 + [here],
        out_shape=[jax.ShapeDtypeStruct(full, jnp.float32)] * 3 + [jax.ShapeDtypeStruct((rows, width), jnp.bfloat16)],
        input_output_aliases={n_in + j: j for j in range(len(held))},
        cost_estimate=pl.CostEstimate(flops=20 * rows * width, bytes_accessed=32 * rows * width, transcendentals=2 * rows * width),
        name="adam",
    )(own, *recvs, *state, *held)


def place_kernel(rows, starts, me, *refs):
    out = refs[-1]
    for start, blocks in zip(starts, refs):
        n, _, size = blocks.shape
        for p in range(n):
            out[:, p * rows + start : p * rows + start + size] = blocks[lax.bitwise_xor(me[0], p)]


def gate(x, after):
    return lax.optimization_barrier((x, after))[0]


def send_cotangent(cotangent, tokens, rows, me, share, order):
    k, m = me // GROUP, me % GROUP
    part = tokens // SHARE
    got = {}
    for s in (3, 2, 1):
        pieces = [
            lax.dynamic_slice(cotangent, (share * part, ((k ^ c) * GROUP + (m ^ s)) * rows), (part, rows)) for c in order
        ]
        got[s] = swap(jnp.concatenate(pieces, axis=1), "dp", s)
    return got


def join_shares(mine, across, both, share, rows):
    peers, part, width = mine.shape
    whole = jnp.zeros((peers, SHARE * part, width), mine.dtype)
    for offset, piece in ((0, mine), (2, across), (1, both[0]), (3, both[1])):
        whole = lax.dynamic_update_slice(whole, piece, (0, (share ^ offset) * part, 0))
    return [[whole[s, :, i : i + rows] for s in range(peers)] for i in range(0, width, rows)]


def reduce_over_tensor(accs, n, owned, t, marks):
    n_tensor, size = lax.axis_size("tensor"), accs[0].shape[1]
    if n_tensor & (n_tensor - 1):
        acc = jnp.concatenate(accs)
        grouped = acc.reshape(n, n_tensor, owned, size).transpose(1, 0, 2, 3).astype(jnp.bfloat16)
        return lax.psum_scatter(grouped, "tensor", scatter_dimension=0, tiled=True).reshape(n, owned, size)
    lefts, bit = [acc.reshape(-1, n_tensor, owned, size) for acc in accs], 1
    while bit < n_tensor:
        mine = (t // bit) % 2
        pairs = [left.reshape(left.shape[0], left.shape[1] // 2, 2, owned, size) for left in lefts]
        going = [lax.dynamic_index_in_dim(pair, 1 - mine, 2, keepdims=False).astype(jnp.bfloat16) for pair in pairs]
        going = jnp.concatenate(going)
        marks.append(going)
        came = swap(going, "tensor", bit).astype(jnp.float32)
        lefts, at = [], 0
        for pair in pairs:
            kept = lax.dynamic_index_in_dim(pair, mine, 2, keepdims=False)
            lefts.append(kept + came[at : at + kept.shape[0]])
            at += kept.shape[0]
        bit *= 2
    return jnp.concatenate([left.reshape(-1, owned, size).astype(jnp.bfloat16) for left in lefts])


def exchange_over_dp(blocks, seen, n, direct):
    blocks = {q: blocks[i] for i, q in enumerate(seen)}
    if direct:
        return jnp.stack([blocks[0]] + [swap(blocks[q], "dp", q) for q in range(1, n)])
    bit = n // 2
    while bit:
        going = [q for q in range(n) if q & bit]
        came = swap(jnp.stack([blocks[q] for q in going]), "dp", bit)
        blocks.update({q: came[i] for i, q in enumerate(going)})
        bit //= 2
    return jnp.stack([blocks[q] for q in range(n)])


def local(activations, cotangent, master, moment_one, moment_two, prompts):
    n, n_tensor = lax.axis_size("dp"), lax.axis_size("tensor")
    me, t = lax.axis_index("dp"), lax.axis_index("tensor")
    k, m = me // GROUP, me % GROUP
    n_groups = n // GROUP
    tokens, width = activations.shape
    rows = master.shape[0]
    state = (master, moment_one, moment_two)
    part_width = width // COLUMN_PARTS
    order = [*range(1, n_groups), 0]

    share = t % SHARE
    away = order[:-1]
    got = send_cotangent(cotangent, tokens, rows, me, share, order)

    blocks = [activations[:, j * part_width : (j + 1) * part_width] for j in range(COLUMN_PARTS)]
    ahead = [swap(block, "dp", 1) for block in blocks]
    side = [swap(block, "dp", 2) for block in blocks]
    diagonal = [swap(beside, "dp", 1) for beside in side]

    mine_of = {
        tag: jnp.stack([got[s][:, low:high] for s in (1, 2, 3)])
        for tag, low, high in (("a", 0, len(away) * rows), ("h", len(away) * rows, len(order) * rows))
    }
    across_of = {tag: swap(mine, "tensor", 2) for tag, mine in mine_of.items()}

    def cotangents(tag, across):
        both = swap(jnp.stack([mine_of[tag], across]), "tensor", 1)
        return join_shares(mine_of[tag], across, both, share, rows)

    def group_sum(j, c, cots, after):
        own = lax.dynamic_slice(cotangent, (0, ((k ^ c) * GROUP + m) * rows), (tokens, rows))
        if after is not None:
            own = gate(own, after)
        partial[j] = dot_tokens(own, blocks[j])
        acc = partial[j] + dot_tokens(cots[0], ahead[j]) + dot_tokens(cots[1], side[j])
        return acc + dot_tokens(cots[2], gate(diagonal[j], acc))

    partial = {}
    last = COLUMN_PARTS - 1
    parts = row_parts(rows)
    cots_away = cotangents("a", across_of["a"])
    sent = [group_sum(0, c, cots_away[i], None).astype(jnp.bfloat16) for i, c in enumerate(away)]
    received = {(0, 0): [swap(x, "dp", c * GROUP) for x, c in zip(sent, away)]}
    mark = sent[-1]

    cots_home = cotangents("h", gate(across_of["h"], mark))
    own_sums = [group_sum(0, 0, cots_home[0], mark)]
    for j in range(1, COLUMN_PARTS):
        sums = [group_sum(j, c, cots_away[i], mark) for i, c in enumerate(away)]
        for start, size in parts if j == last else [(0, rows)]:
            sent = [x[start : start + size].astype(jnp.bfloat16) for x in sums]
            received[j, start] = [swap(x, "dp", c * GROUP) for x, c in zip(sent, away)]
        mark, early_mark = sent[-1], partial[1]
        own_sums.append(group_sum(j, 0, cots_home[0], mark))

    seen, held, bit = [0], [prompts], n // 2
    while bit > 1:
        held.append(swap(jnp.concatenate(held) if len(held) > 1 else held[0], "dp", bit))
        if bit > 2:
            held[-1] = gate(held[-1], early_mark)
        seen += [q ^ bit for q in seen]
        bit //= 2
    near = jnp.concatenate(held[:-1])
    far = held[-1]

    near_other = swap(near, "dp", 1)
    mark = own_sums[-1]
    new_state, weights = None, []
    for j in range(last):
        recvs = [gate(x, mark) for x in received[j, 0]]
        *new_state, weight = adam(own_sums[j], recvs, state, new_state, 0, j * part_width)
        weights.append(weight)
    far = gate(far, weights[-1])
    far_other = swap(far, "dp", 1)
    seen += [q ^ 1 for q in seen]

    def early_part(some):
        return [dot_features(some[:, j * part_width : (j + 1) * part_width], weights[j]) for j in range(last)]

    def late_part(some, done, weight, start, size):
        return sum((e[:, start : start + size] for e in done), start=dot_features(some[:, last * part_width :], weight))

    most = jnp.concatenate([near, far, near_other])
    early = early_part(most)
    early_other, mark = None, early[-1]
    owned = prompts.shape[0] // n_tensor
    outs = []
    for i, (start, size) in enumerate(parts):
        recvs = [gate(x, mark) for x in received[last, start]]
        *new_state, weight = adam(own_sums[last], recvs, state, new_state, start, last * part_width)
        acc = late_part(most, early, weight, start, size)
        if early_other is None:
            far_other = gate(far_other, acc)
            early_other = early_part(far_other)
        acc_other = late_part(far_other, early_other, weight, start, size)
        marks = []
        left = reduce_over_tensor([acc, acc_other], n, owned, t, marks)
        mark = marks[0] if marks else acc_other
        outs.append(exchange_over_dp(left, seen, n, n <= 8 and i == len(parts) - 1))
    projected = pl.pallas_call(
        functools.partial(place_kernel, rows, [start for start, _ in parts]),
        in_specs=[pl.BlockSpec(memory_space=pltpu.SMEM)] + [pl.BlockSpec(memory_space=pltpu.VMEM)] * len(outs),
        out_specs=pl.BlockSpec(memory_space=pltpu.VMEM),
        out_shape=jax.ShapeDtypeStruct((owned, n * rows), jnp.bfloat16),
        name="place",
    )(me.reshape(1), *outs)
    return (*new_state, projected)


def solution(mesh):
    placed = (
        P("dp", "tensor"),
        P("dp", None),
        P("dp", "tensor"),
        P("dp", "tensor"),
        P("dp", "tensor"),
        P("dp", "tensor"),
    )
    return jax.shard_map(
        local,
        mesh=mesh,
        in_specs=placed,
        out_specs=(
            P("dp", "tensor"),
            P("dp", "tensor"),
            P("dp", "tensor"),
            P(("dp", "tensor"), None),
        ),
        check_vma=False,
    )
```
